32 devices in a mesh: data: 4 (over y, z), seq: 8 (over x, core).
Axes of the slice: x: 4, y: 2, z: 2, core: 2. Of those that a mesh axis runs over, the one named last changes fastest.
The devices are a block of a 4x4x8 slice.
Arguments:
- tokens: bfloat16 [32, 256, 384], P('data', 'seq'), parts along dimension 0
- lengths: int32 [32], P('data'), parts along dimension 0
- slot_param: bfloat16 [384, 512], replicated
- logit_scale: float32 [], replicated
- w_in: bfloat16 [256, 384, 1536], P('seq')
- w_out: bfloat16 [256, 1536, 384], P('seq')
Outputs:
- output: bfloat16 [32, 256, 384], P('data', 'seq'), parts along dimension 0
There are 4 independent parts. The reference program is written for one: setup_inputs(seed, part) draws one part's arguments, and reference() takes and returns one part's arrays. A program takes and returns all parts, laid end to end along the dimension named above; an argument that names none is the same for every part.
All inputs are finite; a program needn't handle non-finite values.
Results may differ from the reference program's by a relative error of at most 0.0171172.
Values are sent between devices in bfloat16 or wider.
A program may use at most 768 MiB of HBM per device.

```python
import jax
import jax.numpy as jnp
from jax import lax

BATCH = 8
TOKENS = 256
D_MODEL = 384
FF_DIM = 1536
EXPERTS = 256
SLOTS = 2
LATENT = 16

N_SLOTS = EXPERTS * SLOTS
EPSILON = 1e-6
NEG_FILL = -1e30


def setup_inputs(seed: int = 0, part: int = 0) -> dict:
    shared = jax.random.split(jax.random.key(seed), 6)
    own = jax.random.split(jax.random.fold_in(jax.random.key(seed + 1), part), 3)
    basis = jax.random.normal(shared[0], (LATENT, D_MODEL), jnp.float32)
    phi_code = jax.random.normal(shared[1], (LATENT, N_SLOTS), jnp.float32)
    slot_param = jnp.dot(basis.T, phi_code) / LATENT ** 0.5 + 0.5 * jax.random.normal(shared[2], (D_MODEL, N_SLOTS), jnp.float32)
    logit_scale = 6.0 + 4.0 * jax.random.uniform(shared[3], (), jnp.float32)
    w_in = 2.0 * D_MODEL ** -0.5 * jax.random.normal(shared[4], (EXPERTS, D_MODEL, FF_DIM), jnp.float32)
    w_out = 2.0 * FF_DIM ** -0.5 * jax.random.normal(shared[5], (EXPERTS, FF_DIM, D_MODEL), jnp.float32)
    tok_code = jax.random.normal(own[0], (BATCH, TOKENS, LATENT), jnp.float32)
    tokens = jnp.einsum("btl,ld->btd", tok_code, basis) / LATENT ** 0.5 + 0.5 * jax.random.normal(own[1], (BATCH, TOKENS, D_MODEL), jnp.float32)
    drawn = jax.random.randint(own[2], (BATCH,), 1, TOKENS + 1, jnp.int32)
    lengths = jnp.where(jnp.arange(BATCH) == 0, TOKENS, drawn).astype(jnp.int32)
    return {"tokens": tokens.astype(jnp.bfloat16), "lengths": lengths, "slot_param": slot_param.astype(jnp.bfloat16), "logit_scale": logit_scale, "w_in": w_in.astype(jnp.bfloat16), "w_out": w_out.astype(jnp.bfloat16)}


def l2_normed(values, axis_dim):
    v32 = values.astype(jnp.float32)
    return (v32 * lax.rsqrt(jnp.sum(v32 * v32, axis=axis_dim, keepdims=True) + EPSILON)).astype(jnp.bfloat16)


def reference(tokens, lengths, slot_param, logit_scale, w_in, w_out):
    phi_norm = l2_normed(slot_param, 0).astype(jnp.float32)
    positions = jnp.arange(TOKENS, dtype=jnp.int32)

    def row_logits(tok_row):
        tok_norm = l2_normed(tok_row, 1).astype(jnp.float32)
        return logit_scale * jnp.dot(tok_norm, phi_norm, preferred_element_type=jnp.float32)

    def dispatch_row(row_args):
        tok_row, len_row = row_args
        logits = row_logits(tok_row)
        masked = jnp.where((positions < len_row)[:, None], logits, NEG_FILL)
        disp_w = jnp.exp(masked - jnp.max(masked, axis=0, keepdims=True))
        col_sum = jnp.sum(disp_w, axis=0)
        slot_sum = jnp.dot(disp_w.astype(jnp.bfloat16).astype(jnp.float32).T, tok_row.astype(jnp.float32), preferred_element_type=jnp.float32)
        return (slot_sum / col_sum[:, None]).astype(jnp.bfloat16)

    slot_in = lax.map(dispatch_row, (tokens, lengths))
    slot_grp = jnp.transpose(slot_in.reshape(BATCH, EXPERTS, SLOTS, D_MODEL), (1, 0, 2, 3))

    def expert_ffn(exp_args):
        slot_exp, win_exp, wout_exp = exp_args
        hidden = jnp.einsum("bsd,df->bsf", slot_exp.astype(jnp.float32), win_exp.astype(jnp.float32))
        hidden = jax.nn.gelu(hidden).astype(jnp.bfloat16)
        return jnp.einsum("bsf,fd->bsd", hidden.astype(jnp.float32), wout_exp.astype(jnp.float32)).astype(jnp.bfloat16)

    slot_out = lax.map(expert_ffn, (slot_grp, w_in, w_out))
    slot_out = jnp.transpose(slot_out, (1, 0, 2, 3)).reshape(BATCH, N_SLOTS, D_MODEL)

    def combine_row(row_args):
        tok_row, len_row, out_row = row_args
        logits = row_logits(tok_row)
        comb_w = jnp.exp(logits - jnp.max(logits, axis=1, keepdims=True))
        row_sum = jnp.sum(comb_w, axis=1, keepdims=True)
        tok_mixed = jnp.dot(comb_w.astype(jnp.bfloat16).astype(jnp.float32), out_row.astype(jnp.float32), preferred_element_type=jnp.float32) / row_sum
        return jnp.where((positions < len_row)[:, None], tok_mixed, 0.0).astype(jnp.bfloat16)

    return lax.map(combine_row, (tokens, lengths, slot_out))
```

```python
import functools

import jax
import jax.numpy as jnp
from jax import lax
from jax.experimental import pallas as pl
from jax.experimental.pallas import tpu as pltpu
from jax.sharding import PartitionSpec as P

EPSILON = 1e-6
NEG_FILL = -1e30
F32 = jnp.float32
BF16 = jnp.bfloat16
LANES = 128

OWN_R, OWN_L, OWN_P, FWD_R, FWD_L, L_TO_P, R_TO_P, FR_TO_P, FL_TO_P = range(9)
KINDS = 9

W_SLOTS = 22
CHUNK = 4
SEQ_CHUNK = 2
LAG1 = 4
LAG2 = 7


def unit(values, axis):
    v = values.astype(F32)
    return v * lax.rsqrt(jnp.sum(v * v, axis=axis, keepdims=True) + EPSILON)


def kernel(n_dev, tok, lens, phi, gain, w_in, w_out, out,
           xg, yg, w1, w2, xs, pnt, cexp, hid, rowinv,
           sem1, sem2, tsend, trecv, ysend, yrecv):
    n_seq, n_tok, d_model = tok.shape
    n_exp = w_in.shape[0]
    n_slot = phi.shape[1]
    per_dev = n_slot // n_dev
    per_exp = per_dev // n_exp
    rows = n_seq * per_exp
    n_chunk = n_exp // CHUNK
    n_tchunk = n_seq // SEQ_CHUNK
    n_chip = n_dev // 2
    all_tok = n_dev * n_tok
    own_tok = n_seq * n_tok

    me = lax.axis_index("seq")
    chip, core = me // 2, lax.rem(me, 2)
    right = lax.rem(chip + 1, n_chip) * 2 + core
    left = lax.rem(chip + n_chip - 1, n_chip) * 2 + core
    far = lax.rem(chip + 2, n_chip) * 2 + core
    partner = chip * 2 + 1 - core
    g = gain[0]

    def w1_copy(e, slot):
        return pltpu.make_async_copy(w_in.at[e], w1.at[slot], sem1.at[slot])

    def w2_copy(e, slot):
        return pltpu.make_async_copy(w_out.at[e], w2.at[slot], sem2.at[slot])

    for e in range(W_SLOTS):
        w1_copy(e, e).start()
        w2_copy(e, e).start()

    barrier = pltpu.get_barrier_semaphore()
    for peer in (right, left, partner):
        pl.semaphore_signal(barrier, inc=1, device_id={"seq": peer}, device_id_type=pl.DeviceIdType.MESH)
    pl.semaphore_wait(barrier, 3)

    dest = {OWN_R: right, OWN_L: left, FWD_R: right, FWD_L: left}
    half = SEQ_CHUNK // 2
    ehalf = CHUNK // 2

    def tcopy(kind, k):
        origin = {OWN_R: me, OWN_L: me, OWN_P: me, FWD_R: left, FWD_L: right, L_TO_P: left, R_TO_P: right, FR_TO_P: far, FL_TO_P: far}[kind]
        lo, num = k * SEQ_CHUNK, SEQ_CHUNK
        if kind in (FWD_R, FR_TO_P):
            num = half
        if kind in (FWD_L, FL_TO_P):
            lo, num = lo + half, half
        dst = xg.at[pl.ds(lo, num), origin]
        src = tok.at[pl.ds(lo, num)] if kind in (OWN_R, OWN_L, OWN_P) else dst
        return pltpu.make_async_remote_copy(src_ref=src, dst_ref=dst, send_sem=tsend.at[kind, k], recv_sem=trecv.at[kind, k],
                                            device_id={"seq": dest.get(kind, partner)}, device_id_type=pl.DeviceIdType.MESH)

    def ycopy(kind, k):
        origin = {OWN_R: me, OWN_L: me, OWN_P: me, FWD_R: left, FWD_L: right, L_TO_P: left, R_TO_P: right, FR_TO_P: far, FL_TO_P: far}[kind]
        lo, num = 0, CHUNK
        if kind in (FWD_R, FR_TO_P):
            num = ehalf
        if kind in (FWD_L, FL_TO_P):
            lo, num = ehalf, ehalf
        ref = yg.at[k, origin, pl.ds(lo, num)]
        return pltpu.make_async_remote_copy(src_ref=ref, dst_ref=ref, send_sem=ysend.at[kind, k], recv_sem=yrecv.at[kind, k],
                                            device_id={"seq": dest.get(kind, partner)}, device_id_type=pl.DeviceIdType.MESH)

    def send_own(copy, k):
        for kind in (OWN_R, OWN_L, OWN_P):
            copy(kind, k).start()

    def relay_near(copy, k):
        copy(OWN_R, k).wait_recv()
        copy(FWD_R, k).start()
        copy(L_TO_P, k).start()
        copy(OWN_L, k).wait_recv()
        copy(FWD_L, k).start()
        copy(R_TO_P, k).start()

    def relay_far(copy, k):
        copy(FWD_R, k).wait_recv()
        copy(FR_TO_P, k).start()
        copy(FWD_L, k).wait_recv()
        copy(FL_TO_P, k).start()

    def wait_partner(copy, k):
        for kind in (OWN_P, L_TO_P, R_TO_P, FR_TO_P, FL_TO_P):
            copy(kind, k).wait_recv()

    def wait_sends(copy, k):
        for kind in range(KINDS):
            copy(kind, k).wait_send()

    for k in range(n_tchunk):
        send_own(tcopy, k)

    for b in range(n_seq):
        xg[b, me] = tok[b]

    pn32 = unit(phi[...], 0)
    pn = pn32.astype(BF16)
    slabs = d_model // LANES
    pnt32 = pn.astype(F32).T
    for j in range(slabs):
        pnt[j] = pnt32[:, j * LANES:(j + 1) * LANES]

    def strided_rows(ref, start, size, stride):
        return jnp.concatenate([ref[j, pl.ds(start, size, stride=stride), :] for j in range(slabs)], axis=1)

    own_rows = jnp.concatenate([strided_rows(pnt, me * per_dev + s, n_exp, per_exp) for s in range(per_exp)], axis=0).astype(BF16)

    relay_near(tcopy, 0)

    own = tok[...].reshape(own_tok, d_model)
    own_unit = unit(own, 1).astype(BF16)
    logits = g * jnp.dot(own_unit, pn, preferred_element_type=F32)
    comb = jnp.exp(logits - jnp.max(logits, axis=1, keepdims=True))
    rowinv[...] = 1.0 / jnp.sum(comb, axis=1, keepdims=True)
    comb = comb.astype(BF16)

    relay_near(tcopy, 1)
    relay_far(tcopy, 0)

    width = 256
    devs = width // (CHUNK * rows)
    src = lax.broadcasted_iota(jnp.int32, (devs * per_dev, width), 0)
    col = lax.broadcasted_iota(jnp.int32, (devs * per_dev, width), 1)
    base = col // (CHUNK * rows) * per_dev + lax.rem(col, CHUNK * rows) // rows * per_exp + lax.rem(col, per_exp)
    row_seq = lax.broadcasted_iota(jnp.int32, (own_tok, width), 0) // n_tok
    col_seq = lax.rem(lax.broadcasted_iota(jnp.int32, (own_tok, width), 1), rows) // per_exp
    same = row_seq == col_seq

    def spread(k):
        pick = (src == base + k * (CHUNK * per_exp)).astype(F32).astype(BF16)
        for d in range(n_dev // devs):
            part = jnp.dot(comb[:, d * devs * per_dev:(d + 1) * devs * per_dev], pick, preferred_element_type=F32)
            cexp[k, :, d * width:(d + 1) * width] = jnp.where(same, part, 0.0).astype(BF16)

    for k in range(n_chunk // 2):
        spread(k)
    relay_near(tcopy, 2)
    relay_far(tcopy, 1)
    for k in range(n_chunk // 2, n_chunk):
        spread(k)
    relay_near(tcopy, 3)
    relay_far(tcopy, 2)

    pos = lax.broadcasted_iota(jnp.int32, (per_dev, all_tok), 1)

    def dispatch(b):
        x = xg[b].reshape(all_tok, d_model)
        xn = unit(x, 1).astype(BF16)
        lt = g * lax.dot_general(own_rows, xn, (((1,), (1,)), ((), ())), preferred_element_type=F32)
        lt = jnp.where(pos < lens[b], lt, NEG_FILL)
        e = jnp.exp(lt - jnp.max(lt, axis=1, keepdims=True))
        z = jnp.sum(e, axis=1, keepdims=True)
        s = jnp.dot(e.astype(BF16), x, preferred_element_type=F32) / z
        s = s.astype(BF16).astype(F32)
        for j in range(slabs):
            xs[j, b * per_dev:(b + 1) * per_dev, :] = s[:, j * LANES:(j + 1) * LANES]

    for k in range(n_tchunk):
        if k == n_tchunk - 1:
            relay_far(tcopy, k)
        wait_partner(tcopy, k)
        for b in range(k * SEQ_CHUNK, (k + 1) * SEQ_CHUNK):
            dispatch(b)

    def up(e, slot, u):
        x = strided_rows(xs, e, rows, n_exp).astype(BF16)
        hid[u] = jax.nn.gelu(jnp.dot(x, w1[slot], preferred_element_type=F32)).astype(BF16)

    def down(k, e, u):
        slot = lax.rem(e, W_SLOTS)
        yg[k, me, u] = jnp.dot(hid[u], w2[slot], preferred_element_type=F32).astype(BF16)

    for u in range(CHUNK):
        w1_copy(u, u).wait()
    for u in range(CHUNK):
        up(u, u, u)
    for u in range(CHUNK):
        if u + W_SLOTS < n_exp:
            w1_copy(u + W_SLOTS, u).start()

    def comm(k):
        send_own(ycopy, k - 1)

        @pl.when(k >= LAG1)
        def _():
            relay_near(ycopy, k - LAG1)

        @pl.when(k >= LAG2)
        def _():
            relay_far(ycopy, k - LAG2)

    def step(k, carry):
        first = k * CHUNK

        @pl.when(k >= 1)
        def _():
            comm(k)

        last = k == n_chunk - 1
        for u in range(CHUNK):
            e = first + u
            w2_copy(e, lax.rem(e, W_SLOTS)).wait()

            @pl.when(jnp.logical_not(last))
            def _():
                w1_copy(e + CHUNK, lax.rem(e + CHUNK, W_SLOTS)).wait()
        for u in range(CHUNK):
            down(k, first + u, u)
        for u in range(CHUNK):
            e = jnp.minimum(first + CHUNK + u, n_exp - 1)
            up(e, lax.rem(e, W_SLOTS), u)
        for u in range(CHUNK):
            e = first + u

            @pl.when(e + W_SLOTS < n_exp)
            def _():
                w2_copy(e + W_SLOTS, lax.rem(e, W_SLOTS)).start()

            @pl.when(e + CHUNK + W_SLOTS < n_exp)
            def _():
                w1_copy(e + CHUNK + W_SLOTS, lax.rem(e + CHUNK, W_SLOTS)).start()
        return carry

    lax.fori_loop(0, n_chunk, step, 0)

    acc = jnp.zeros((own_tok, d_model), F32)

    def combine(acc, k):
        wait_partner(ycopy, k)
        y = yg[k].reshape(n_dev * CHUNK * rows, d_model)
        return acc + jnp.dot(cexp[k], y, preferred_element_type=F32)

    send_own(ycopy, n_chunk - 1)
    for k in range(n_chunk, n_chunk + LAG2):
        if 0 <= k - LAG1 < n_chunk:
            relay_near(ycopy, k - LAG1)
        if 0 <= k - LAG2 < n_chunk:
            relay_far(ycopy, k - LAG2)
        if 0 <= k - LAG2 - 1 < n_chunk:
            acc = combine(acc, k - LAG2 - 1)
    acc = combine(acc, n_chunk - 1)

    y = (acc * rowinv[...]).reshape(n_seq, n_tok, d_model)
    tpos = lax.broadcasted_iota(jnp.int32, (n_tok, d_model), 0) + me * n_tok
    for b in range(n_seq):
        out[b] = jnp.where(tpos < lens[b], y[b], 0.0).astype(BF16)

    for k in range(n_tchunk):
        wait_sends(tcopy, k)
    for k in range(n_chunk):
        wait_sends(ycopy, k)


def solution(mesh):
    n_dev = mesh.shape["seq"]

    def local_layer(tok_blk, len_blk, slot_param, logit_scale, w_in, w_out):
        n_seq, n_tok, d_model = tok_blk.shape
        n_exp, _, d_ff = w_in.shape
        n_slot = slot_param.shape[1]
        per_exp = n_slot // n_dev // n_exp
        rows = n_seq * per_exp
        n_chunk = n_exp // CHUNK
        vmem = pl.BlockSpec(memory_space=pltpu.VMEM)
        smem = pl.BlockSpec(memory_space=pltpu.SMEM)
        hbm = pl.BlockSpec(memory_space=pl.ANY)
        return pl.pallas_call(
            functools.partial(kernel, n_dev),
            out_shape=jax.ShapeDtypeStruct(tok_blk.shape, BF16),
            in_specs=[vmem, smem, vmem, smem, hbm, hbm],
            out_specs=vmem,
            scratch_shapes=[
                pltpu.VMEM((n_seq, n_dev, n_tok, d_model), BF16),
                pltpu.VMEM((n_chunk, n_dev, CHUNK, rows, d_model), BF16),
                pltpu.VMEM((W_SLOTS, d_model, d_ff), BF16),
                pltpu.VMEM((W_SLOTS, d_ff, d_model), BF16),
                pltpu.VMEM((d_model // LANES, n_slot, LANES), F32),
                pltpu.VMEM((d_model // LANES, n_slot, LANES), F32),
                pltpu.VMEM((n_chunk, n_seq * n_tok, n_dev * CHUNK * rows), BF16),
                pltpu.VMEM((CHUNK, rows, d_ff), BF16),
                pltpu.VMEM((n_seq * n_tok, 1), F32),
                pltpu.SemaphoreType.DMA((W_SLOTS,)),
                pltpu.SemaphoreType.DMA((W_SLOTS,)),
                pltpu.SemaphoreType.DMA((KINDS, n_seq // SEQ_CHUNK)),
                pltpu.SemaphoreType.DMA((KINDS, n_seq // SEQ_CHUNK)),
                pltpu.SemaphoreType.DMA((KINDS, n_chunk)),
                pltpu.SemaphoreType.DMA((KINDS, n_chunk)),
            ],
            compiler_params=pltpu.CompilerParams(collective_id=0, has_side_effects=True, vmem_limit_bytes=67000000),
            name="soft_moe",
        )(tok_blk, len_blk, slot_param, logit_scale.reshape(1), w_in, w_out)

    return jax.shard_map(local_layer, mesh=mesh, in_specs=(P("data", "seq", None), P("data"), P(None, None), P(), P("seq", None, None), P("seq", None, None)), out_specs=P("data", "seq", None), check_vma=False)
```

```python
import functools

import jax
import jax.numpy as jnp
from jax import lax
from jax.experimental import pallas as pl
from jax.experimental.pallas import tpu as pltpu
from jax.sharding import PartitionSpec as P

EPSILON = 1e-6
NEG_FILL = -1e30
F32 = jnp.float32
BF16 = jnp.bfloat16
LANES = 128
MESH = pl.DeviceIdType.MESH

OWN_R, OWN_L, OWN_P, FWD_R, FWD_L, L_TO_P, R_TO_P, FAR_TO_P = range(8)
UNITS_SENT = 7
UNITS_FROM_PARTNER = 4
FROM_LEFT, FROM_RIGHT, FAR, PARTNER = range(4)
RECV = {OWN_R: FROM_LEFT, OWN_L: FROM_RIGHT, FWD_R: FAR, FWD_L: FAR}

CHUNK = 4
W_SLOTS = 5
SEQ_CHUNK = 2
LAG = 4


def unit(values, axis):
    v = values.astype(F32)
    return v * lax.rsqrt(jnp.sum(v * v, axis=axis, keepdims=True) + EPSILON)


def kernel(n_dev, tok_hbm, lens_hbm, phi_hbm, gain, w_in, w_out, out,
           tok, phi, lens, xg, yg, w1, w2, xs, pnt, cexp, hid, rowinv,
           insem, sem1, sem2, tsend, trecv, ysend, yrecv):
    n_seq, n_tok, d_model = tok.shape
    n_exp = w_in.shape[0]
    n_slot = phi.shape[1]
    per_dev = n_slot // n_dev
    per_exp = per_dev // n_exp
    rows = n_seq * per_exp
    n_chunk = n_exp // CHUNK
    n_tchunk = n_seq // SEQ_CHUNK
    n_chip = n_dev // 2
    all_tok = n_dev * n_tok
    own_tok = n_seq * n_tok
    slabs = d_model // LANES

    me = lax.axis_index("seq")
    chip, core = me // 2, lax.rem(me, 2)
    right = lax.rem(chip + 1, n_chip) * 2 + core
    left = lax.rem(chip + n_chip - 1, n_chip) * 2 + core
    far = lax.rem(chip + 2, n_chip) * 2 + core
    partner = chip * 2 + 1 - core

    barrier = pltpu.get_barrier_semaphore()
    for peer in (right, left, partner):
        pl.semaphore_signal(barrier, inc=1, device_id={"seq": peer}, device_id_type=MESH)

    tok_in = pltpu.make_async_copy(tok_hbm, tok, insem.at[0])
    phi_in = pltpu.make_async_copy(phi_hbm, phi, insem.at[1])
    lens_in = pltpu.make_async_copy(lens_hbm, lens, insem.at[2])
    tok_in.start()
    phi_in.start()
    lens_in.start()

    def w1_copy(k, slot):
        return pltpu.make_async_copy(w_in.at[pl.ds(k * CHUNK, CHUNK)], w1.at[slot], sem1.at[slot])

    def w2_copy(k, slot):
        return pltpu.make_async_copy(w_out.at[pl.ds(k * CHUNK, CHUNK)], w2.at[slot], sem2.at[slot])

    for k in range(W_SLOTS):
        w1_copy(k, k).start(priority=1)
        w2_copy(k, k).start(priority=1)

    dest = {OWN_R: right, OWN_L: left, FWD_R: right, FWD_L: left}
    origins = {FWD_R: left, FWD_L: right, L_TO_P: left, R_TO_P: right, FAR_TO_P: far}

    def part(kind, size):
        if kind == FWD_R:
            return 0, size // 2
        if kind == FWD_L:
            return size // 2, size // 2
        return 0, size

    def remote(src, dst, send_sem, recv_sem, device):
        return pltpu.make_async_remote_copy(src_ref=src, dst_ref=dst, send_sem=send_sem, recv_sem=recv_sem,
                                            device_id={"seq": device}, device_id_type=MESH)

    class Tokens:
        def send(kind, k):
            lo, num = part(kind, SEQ_CHUNK)
            lo = lo + k * SEQ_CHUNK
            dst = xg.at[pl.ds(lo, num), origins.get(kind, me)]
            src = dst if kind in origins else tok.at[pl.ds(lo, num)]
            remote(src, dst, tsend, trecv.at[RECV.get(kind, PARTNER), k], dest.get(kind, partner)).start()

        def arrived(what, k):
            units = UNITS_FROM_PARTNER if what == PARTNER else 1
            ref = xg.at[pl.ds(k * SEQ_CHUNK, SEQ_CHUNK), pl.ds(0, units)]
            remote(ref, ref, tsend, trecv.at[what, k], partner).wait_recv()

        def all_sent():
            ref = xg.at[:, pl.ds(0, UNITS_SENT)]
            remote(ref, ref, tsend, trecv.at[0, 0], partner).wait_send()

    class Slots:
        def send(kind, k):
            lo, num = part(kind, CHUNK)
            ref = yg.at[k, origins.get(kind, me), pl.ds(lo, num)]
            remote(ref, ref, ysend, yrecv.at[RECV.get(kind, PARTNER), k], dest.get(kind, partner)).start()

        def arrived(what, k):
            units = UNITS_FROM_PARTNER if what == PARTNER else 1
            ref = yg.at[k, pl.ds(0, units)]
            remote(ref, ref, ysend, yrecv.at[what, k], partner).wait_recv()

        def all_sent():
            ref = yg.at[:, pl.ds(0, UNITS_SENT)]
            remote(ref, ref, ysend, yrecv.at[0, 0], partner).wait_send()

    def send_own(gather, k):
        for kind in (OWN_R, OWN_L, OWN_P):
            gather.send(kind, k)

    def relay_near(gather, k):
        gather.arrived(FROM_LEFT, k)
        gather.send(FWD_R, k)
        gather.send(L_TO_P, k)
        gather.arrived(FROM_RIGHT, k)
        gather.send(FWD_L, k)
        gather.send(R_TO_P, k)

    def relay_far(gather, k):
        gather.arrived(FAR, k)
        gather.send(FAR_TO_P, k)

    tok_in.wait()
    pl.semaphore_wait(barrier, 3)
    for k in range(n_tchunk):
        send_own(Tokens, k)

    for b in range(n_seq):
        xg[b, me] = tok[b]

    phi_in.wait()
    lens_in.wait()
    g = gain[0]
    pn = unit(phi[...], 0).astype(BF16)
    pnt32 = pn.astype(F32).T
    for j in range(slabs):
        pnt[j] = pnt32[:, j * LANES:(j + 1) * LANES]

    def strided_rows(ref, start, size, stride):
        return jnp.concatenate([ref[j, pl.ds(start, size, stride=stride), :] for j in range(slabs)], axis=1)

    own_rows = jnp.concatenate([strided_rows(pnt, me * per_dev + s, n_exp, per_exp) for s in range(per_exp)], axis=0).astype(BF16)

    own = tok[...].reshape(own_tok, d_model)
    own_unit = unit(own, 1).astype(BF16)
    logits = g * jnp.dot(own_unit, pn, preferred_element_type=F32)
    comb = jnp.exp(logits - jnp.max(logits, axis=1, keepdims=True))
    rowinv[...] = 1.0 / jnp.sum(comb, axis=1, keepdims=True)
    comb = comb.astype(BF16)

    relay_near(Tokens, 0)

    width = 256
    devs = width // (CHUNK * rows)
    src = lax.broadcasted_iota(jnp.int32, (devs * per_dev, width), 0)
    col = lax.broadcasted_iota(jnp.int32, (devs * per_dev, width), 1)
    base = col // (CHUNK * rows) * per_dev + lax.rem(col, CHUNK * rows) // rows * per_exp + lax.rem(col, per_exp)
    row_seq = lax.broadcasted_iota(jnp.int32, (own_tok, width), 0) // n_tok
    col_seq = lax.rem(lax.broadcasted_iota(jnp.int32, (own_tok, width), 1), rows) // per_exp
    same = row_seq == col_seq

    def spread(k):
        pick = (src == base + k * (CHUNK * per_exp)).astype(F32).astype(BF16)
        for d in range(n_dev // devs):
            piece = jnp.dot(comb[:, d * devs * per_dev:(d + 1) * devs * per_dev], pick, preferred_element_type=F32)
            cexp[k, :, d * width:(d + 1) * width] = jnp.where(same, piece, 0.0).astype(BF16)

    share = n_chunk // (n_tchunk - 1)
    for t in range(1, n_tchunk):
        for k in range((t - 1) * share, n_chunk if t == n_tchunk - 1 else t * share):
            spread(k)
        relay_near(Tokens, t)

    pos = lax.broadcasted_iota(jnp.int32, (per_dev, all_tok), 1)

    def dispatch(b):
        x = xg[b].reshape(all_tok, d_model)
        xn = unit(x, 1).astype(BF16)
        lt = g * lax.dot_general(own_rows, xn, (((1,), (1,)), ((), ())), preferred_element_type=F32)
        lt = jnp.where(pos < lens[b], lt, NEG_FILL)
        e = jnp.exp(lt - jnp.max(lt, axis=1, keepdims=True))
        z = jnp.sum(e, axis=1, keepdims=True)
        s = jnp.dot(e.astype(BF16), x, preferred_element_type=F32) / z
        s = s.astype(BF16).astype(F32)
        for j in range(slabs):
            xs[j, b * per_dev:(b + 1) * per_dev, :] = s[:, j * LANES:(j + 1) * LANES]

    def dispatch_chunks(first, last):
        for k in range(first, last):
            Tokens.arrived(PARTNER, k)
        for b in range(first * SEQ_CHUNK, last * SEQ_CHUNK):
            dispatch(b)

    for k in range(n_tchunk):
        relay_far(Tokens, k)
    dispatch_chunks(0, n_tchunk // 2)
    dispatch_chunks(n_tchunk // 2, n_tchunk)

    def up(k, slot):
        for u in range(CHUNK):
            x = strided_rows(xs, k * CHUNK + u, rows, n_exp).astype(BF16)
            hid[u] = jax.nn.gelu(jnp.dot(x, w1[slot, u], preferred_element_type=F32)).astype(BF16)

    def down(k, slot):
        for u in range(CHUNK):
            yg[k, me, u] = jnp.dot(hid[u], w2[slot, u], preferred_element_type=F32).astype(BF16)

    w1_copy(0, 0).wait()
    up(0, 0)
    w1_copy(W_SLOTS, 0).start(priority=1)

    def step(k, carry):
        @pl.when(k >= 1)
        def _():
            send_own(Slots, k - 1)

        @pl.when(k >= LAG)
        def _():
            relay_near(Slots, k - LAG)

        slot, after = lax.rem(k, W_SLOTS), lax.rem(k + 1, W_SLOTS)
        w2_copy(k, slot).wait()
        w1_copy(k + 1, after).wait()
        down(k, slot)
        up(k + 1, after)

        @pl.when(k + W_SLOTS < n_chunk)
        def _():
            w2_copy(k + W_SLOTS, slot).start(priority=1)

        @pl.when(k + 1 + W_SLOTS < n_chunk)
        def _():
            w1_copy(k + 1 + W_SLOTS, after).start(priority=1)
        return carry

    lax.fori_loop(0, n_chunk - 1, step, 0)
    last = n_chunk - 1
    send_own(Slots, last - 1)
    w2_copy(last, last % W_SLOTS).wait()
    down(last, last % W_SLOTS)

    acc = jnp.zeros((own_tok, d_model), F32)

    def combine(acc, k):
        Slots.arrived(PARTNER, k)
        y = yg[k].reshape(n_dev * CHUNK * rows, d_model)
        return acc + jnp.dot(cexp[k], y, preferred_element_type=F32)

    first = last - LAG
    relay_near(Slots, first)
    send_own(Slots, last)
    far_done = comb_done = 0
    for k in range(first + 1, n_chunk):
        relay_near(Slots, k)
        for _ in range(2):
            if far_done < first - 1:
                relay_far(Slots, far_done)
                far_done += 1
                if far_done >= 3:
                    acc = combine(acc, comb_done)
                    comb_done += 1
    while far_done < n_chunk:
        relay_far(Slots, far_done)
        far_done += 1
        if far_done >= comb_done + 3:
            acc = combine(acc, comb_done)
            comb_done += 1
    while comb_done < n_chunk:
        acc = combine(acc, comb_done)
        comb_done += 1

    y = (acc * rowinv[...]).reshape(n_seq, n_tok, d_model)
    tpos = lax.broadcasted_iota(jnp.int32, (n_tok, d_model), 0) + me * n_tok
    for b in range(n_seq):
        out[b] = jnp.where(tpos < lens[b], y[b], 0.0).astype(BF16)

    Tokens.all_sent()
    Slots.all_sent()


def solution(mesh):
    n_dev = mesh.shape["seq"]

    def local_layer(tok_blk, len_blk, slot_param, logit_scale, w_in, w_out):
        n_seq, n_tok, d_model = tok_blk.shape
        n_exp, _, d_ff = w_in.shape
        n_slot = slot_param.shape[1]
        per_exp = n_slot // n_dev // n_exp
        rows = n_seq * per_exp
        n_chunk = n_exp // CHUNK
        vmem = pl.BlockSpec(memory_space=pltpu.VMEM)
        smem = pl.BlockSpec(memory_space=pltpu.SMEM)
        hbm = pl.BlockSpec(memory_space=pl.ANY)
        return pl.pallas_call(
            functools.partial(kernel, n_dev),
            out_shape=jax.ShapeDtypeStruct(tok_blk.shape, BF16),
            in_specs=[hbm, hbm, hbm, smem, hbm, hbm],
            out_specs=vmem,
            scratch_shapes=[
                pltpu.VMEM(tok_blk.shape, BF16),
                pltpu.VMEM(slot_param.shape, BF16),
                pltpu.SMEM(len_blk.shape, jnp.int32),
                pltpu.VMEM((n_seq, n_dev, n_tok, d_model), BF16),
                pltpu.VMEM((n_chunk, n_dev, CHUNK, rows, d_model), BF16),
                pltpu.VMEM((W_SLOTS, CHUNK, d_model, d_ff), BF16),
                pltpu.VMEM((W_SLOTS, CHUNK, d_ff, d_model), BF16),
                pltpu.VMEM((d_model // LANES, n_slot, LANES), F32),
                pltpu.VMEM((d_model // LANES, n_slot, LANES), F32),
                pltpu.VMEM((n_chunk, n_seq * n_tok, n_dev * CHUNK * rows), BF16),
                pltpu.VMEM((CHUNK, rows, d_ff), BF16),
                pltpu.VMEM((n_seq * n_tok, 1), F32),
                pltpu.SemaphoreType.DMA((3,)),
                pltpu.SemaphoreType.DMA((W_SLOTS,)),
                pltpu.SemaphoreType.DMA((W_SLOTS,)),
                pltpu.SemaphoreType.DMA,
                pltpu.SemaphoreType.DMA((4, n_seq // SEQ_CHUNK)),
                pltpu.SemaphoreType.DMA,
                pltpu.SemaphoreType.DMA((4, n_chunk)),
            ],
            compiler_params=pltpu.CompilerParams(collective_id=0, has_side_effects=True, vmem_limit_bytes=67000000),
            name="soft_moe",
        )(tok_blk, len_blk, slot_param, logit_scale.reshape(1), w_in, w_out)

    return jax.shard_map(local_layer, mesh=mesh, in_specs=(P("data", "seq", None), P("data"), P(None, None), P(), P("seq", None, None), P("seq", None, None)), out_specs=P("data", "seq", None), check_vma=False)
```

```python
import functools

import jax
import jax.numpy as jnp
from jax import lax
from jax.experimental import pallas as pl
from jax.experimental.pallas import tpu as pltpu
from jax.sharding import PartitionSpec as P

EPSILON = 1e-6
NEG_FILL = -1e30
F32 = jnp.float32
BF16 = jnp.bfloat16
LANES = 128
MESH = pl.DeviceIdType.MESH

OWN_R, OWN_L, OWN_P, FWD_R, FWD_L, FWD_R2, FWD_L2, L_TO_P, R_TO_P, FAR_TO_P = range(10)
UNITS_SENT = 7
FROM_LEFT, FROM_RIGHT, FAR, PARTNER, PARTNER_FAR = range(5)
RECV = {OWN_R: FROM_LEFT, OWN_L: FROM_RIGHT, FWD_R: FAR, FWD_L: FAR, FWD_R2: PARTNER_FAR, FWD_L2: PARTNER_FAR, FAR_TO_P: PARTNER_FAR}
UNITS = {PARTNER: 3}
OWN, LEFT, RIGHT, ACROSS = 0, 2, 4, 6
SRC_PLACE = {FWD_R: LEFT, FWD_L: RIGHT, FWD_R2: LEFT, FWD_L2: RIGHT, L_TO_P: LEFT, R_TO_P: RIGHT, FAR_TO_P: ACROSS}
DST_PLACE = {OWN_R: LEFT, OWN_L: RIGHT, OWN_P: OWN + 1, FWD_R: ACROSS, FWD_L: ACROSS, FWD_R2: ACROSS + 1, FWD_L2: ACROSS + 1, L_TO_P: LEFT + 1, R_TO_P: RIGHT + 1, FAR_TO_P: ACROSS + 1}

CHUNK = 4
W_SLOTS = 5
SEQ_CHUNK = 2
TOK_BOTH = 3
SLOT_BOTH = 7
LAG = 4


def unit(values, axis):
    v = values.astype(F32)
    return v * lax.rsqrt(jnp.sum(v * v, axis=axis, keepdims=True) + EPSILON)


def kernel(n_dev, tok_hbm, lens_hbm, phi_hbm, gain, w_in, w_out, out,
           tok, phi, lens, xg, yg, w1, w2, xs, pnt, nlt, cexp, hid, rowinv,
           insem, sem1, sem2, tsend, trecv, ysend, yrecv):
    n_seq, n_tok, d_model = tok.shape
    n_exp = w_in.shape[0]
    n_slot = phi.shape[1]
    per_dev = n_slot // n_dev
    per_exp = per_dev // n_exp
    rows = n_seq * per_exp
    n_chunk = n_exp // CHUNK
    n_tchunk = n_seq // SEQ_CHUNK
    n_chip = n_dev // 2
    own_tok = n_seq * n_tok
    slabs = d_model // LANES

    me = lax.axis_index("seq")
    chip, core = me // 2, lax.rem(me, 2)
    right = lax.rem(chip + 1, n_chip) * 2 + core
    left = lax.rem(chip + n_chip - 1, n_chip) * 2 + core
    far = lax.rem(chip + 2, n_chip) * 2 + core
    partner = chip * 2 + 1 - core

    barrier = pltpu.get_barrier_semaphore()
    other = 1 - 2 * core
    for peer in (right, left, right + other, left + other, partner):
        pl.semaphore_signal(barrier, inc=1, device_id={"seq": peer}, device_id_type=MESH)

    tok_in = pltpu.make_async_copy(tok_hbm, tok, insem.at[0])
    phi_in = pltpu.make_async_copy(phi_hbm, phi, insem.at[1])
    lens_in = pltpu.make_async_copy(lens_hbm, lens, insem.at[2])
    tok_in.start()
    phi_in.start()
    lens_in.start()

    def w1_copy(k, slot):
        return pltpu.make_async_copy(w_in.at[pl.ds(k * CHUNK, CHUNK)], w1.at[slot], sem1.at[slot])

    def w2_copy(k, slot):
        return pltpu.make_async_copy(w_out.at[pl.ds(k * CHUNK, CHUNK)], w2.at[slot], sem2.at[slot])

    for k in range(W_SLOTS):
        w1_copy(k, k).start(priority=1)
        w2_copy(k, k).start(priority=1)

    dest = {OWN_R: right, OWN_L: left, FWD_R: right, FWD_L: left, FWD_R2: right + other, FWD_L2: left + other}
    origins = {FWD_R: left, FWD_L: right, FWD_R2: left, FWD_L2: right, L_TO_P: left, R_TO_P: right, FAR_TO_P: far}

    def part(kind, size):
        if kind in (FWD_R, FWD_R2):
            return 0, size // 2
        if kind in (FWD_L, FWD_L2):
            return size // 2, size // 2
        return 0, size

    def remote(src, dst, send_sem, recv_sem, device):
        return pltpu.make_async_remote_copy(src_ref=src, dst_ref=dst, send_sem=send_sem, recv_sem=recv_sem,
                                            device_id={"seq": device}, device_id_type=MESH)

    class Tokens:
        both = TOK_BOTH

        def send(kind, k):
            lo, num = part(kind, SEQ_CHUNK)
            lo = lo + k * SEQ_CHUNK
            dst = xg.at[pl.ds(lo, num), DST_PLACE[kind]]
            src = xg.at[pl.ds(lo, num), SRC_PLACE[kind]] if kind in SRC_PLACE else tok.at[pl.ds(lo, num)]
            remote(src, dst, tsend, trecv.at[RECV.get(kind, PARTNER), k], dest.get(kind, partner)).start()

        def arrived(what, k):
            ref = xg.at[pl.ds(k * SEQ_CHUNK, SEQ_CHUNK), pl.ds(0, UNITS.get(what, 1))]
            remote(ref, ref, tsend, trecv.at[what, k], partner).wait_recv()

        def all_sent():
            ref = xg.at[:, pl.ds(0, UNITS_SENT)]
            remote(ref, ref, tsend, trecv.at[0, 0], partner).wait_send()

    class Slots:
        both = SLOT_BOTH

        def send(kind, k):
            lo, num = part(kind, CHUNK)
            ref = yg.at[k, origins.get(kind, me), pl.ds(lo, num)]
            remote(ref, ref, ysend, yrecv.at[RECV.get(kind, PARTNER), k], dest.get(kind, partner)).start()

        def arrived(what, k):
            ref = yg.at[k, pl.ds(0, UNITS.get(what, 1))]
            remote(ref, ref, ysend, yrecv.at[what, k], partner).wait_recv()

        def all_sent():
            ref = yg.at[:, pl.ds(0, UNITS_SENT)]
            remote(ref, ref, ysend, yrecv.at[0, 0], partner).wait_send()

    def send_own(gather, k):
        for kind in (OWN_R, OWN_L, OWN_P):
            gather.send(kind, k)

    def relay_near(gather, k):
        both = isinstance(k, int) and k >= gather.both
        gather.arrived(FROM_LEFT, k)
        gather.send(FWD_R, k)
        if both:
            gather.send(FWD_R2, k)
        gather.send(L_TO_P, k)
        gather.arrived(FROM_RIGHT, k)
        gather.send(FWD_L, k)
        if both:
            gather.send(FWD_L2, k)
        gather.send(R_TO_P, k)

    def relay_far(gather, k):
        gather.arrived(FAR, k)
        if k < gather.both:
            gather.send(FAR_TO_P, k)

    tok_in.wait()
    pl.semaphore_wait(barrier, 5)
    for k in range(n_tchunk):
        send_own(Tokens, k)

    for b in range(n_seq):
        xg[b, OWN] = tok[b]

    phi_in.wait()
    lens_in.wait()
    g = gain[0]
    pn = unit(phi[...], 0).astype(BF16)
    pnt32 = pn.astype(F32).T
    for j in range(slabs):
        pnt[j] = pnt32[:, j * LANES:(j + 1) * LANES]

    def strided_rows(ref, start, size, stride):
        return jnp.concatenate([ref[j, pl.ds(start, size, stride=stride), :] for j in range(slabs)], axis=1)

    own_rows = jnp.concatenate([strided_rows(pnt, me * per_dev + s, n_exp, per_exp) for s in range(per_exp)], axis=0).astype(BF16)

    own = tok[...].reshape(own_tok, d_model)
    own_unit = unit(own, 1).astype(BF16)
    logits = g * jnp.dot(own_unit, pn, preferred_element_type=F32)
    comb = jnp.exp(logits - jnp.max(logits, axis=1, keepdims=True))
    rowinv[...] = 1.0 / jnp.sum(comb, axis=1, keepdims=True)
    comb = comb.astype(BF16)

    relay_near(Tokens, 0)

    width = 256
    devs = width // (CHUNK * rows)
    src = lax.broadcasted_iota(jnp.int32, (devs * per_dev, width), 0)
    col = lax.broadcasted_iota(jnp.int32, (devs * per_dev, width), 1)
    base = col // (CHUNK * rows) * per_dev + lax.rem(col, CHUNK * rows) // rows * per_exp + lax.rem(col, per_exp)
    row_seq = lax.broadcasted_iota(jnp.int32, (own_tok, width), 0) // n_tok
    col_seq = lax.rem(lax.broadcasted_iota(jnp.int32, (own_tok, width), 1), rows) // per_exp
    same = row_seq == col_seq

    def spread(k):
        pick = (src == base + k * (CHUNK * per_exp)).astype(F32).astype(BF16)
        for d in range(n_dev // devs):
            piece = jnp.dot(comb[:, d * devs * per_dev:(d + 1) * devs * per_dev], pick, preferred_element_type=F32)
            cexp[k, :, d * width:(d + 1) * width] = jnp.where(same, piece, 0.0).astype(BF16)

    share = n_chunk // (n_tchunk - 1)
    for t in range(1, n_tchunk):
        for k in range((t - 1) * share, n_chunk if t == n_tchunk - 1 else t * share):
            spread(k)
        relay_near(Tokens, t)

    near = ACROSS
    places = (me, partner, left, left + other, right, right + other, far, far + other)

    def positions(first, last):
        lane = lax.broadcasted_iota(jnp.int32, (per_dev, (last - first) * n_tok), 1)
        device = jnp.full(lane.shape, places[first], jnp.int32)
        for r in range(first + 1, last):
            device = jnp.where(lane // n_tok == r - first, places[r], device)
        return device * n_tok + lax.rem(lane, n_tok)

    def part_logits(x, pos, b):
        xn = unit(x, 1).astype(BF16)
        lt = g * lax.dot_general(own_rows, xn, (((1,), (1,)), ((), ())), preferred_element_type=F32)
        return jnp.where(pos < lens[b], lt, NEG_FILL)

    near_pos, far_pos = positions(0, near), positions(near, n_dev)

    def tokens_of(b, first, last):
        return xg[b, first:last].reshape((last - first) * n_tok, d_model)

    def near_logits(k):
        Tokens.arrived(PARTNER, k)
        for b in range(k * SEQ_CHUNK, (k + 1) * SEQ_CHUNK):
            nlt[b] = part_logits(tokens_of(b, 0, near), near_pos, b)

    def dispatch(b):
        lt_n, x_f = nlt[b], tokens_of(b, near, n_dev)
        lt_f = part_logits(x_f, far_pos, b)
        top = jnp.maximum(jnp.max(lt_n, axis=1, keepdims=True), jnp.max(lt_f, axis=1, keepdims=True))
        e_n, e_f = jnp.exp(lt_n - top), jnp.exp(lt_f - top)
        z = jnp.sum(e_n, axis=1, keepdims=True) + jnp.sum(e_f, axis=1, keepdims=True)
        s = jnp.dot(e_n.astype(BF16), tokens_of(b, 0, near), preferred_element_type=F32)
        s = (s + jnp.dot(e_f.astype(BF16), x_f, preferred_element_type=F32)) / z
        s = s.astype(BF16).astype(F32)
        for j in range(slabs):
            xs[j, b * per_dev:(b + 1) * per_dev, :] = s[:, j * LANES:(j + 1) * LANES]

    for k in range(n_tchunk):
        near_logits(k)
        if k == 1:
            relay_far(Tokens, 0)
        if k >= 1:
            relay_far(Tokens, k)
    for k in range(n_tchunk):
        Tokens.arrived(PARTNER_FAR, k)
    for b in range(n_seq):
        dispatch(b)

    def up(k, slot):
        for u in range(CHUNK):
            x = strided_rows(xs, k * CHUNK + u, rows, n_exp).astype(BF16)
            hid[u] = jax.nn.gelu(jnp.dot(x, w1[slot, u], preferred_element_type=F32)).astype(BF16)

    def down(k, slot):
        for u in range(CHUNK):
            yg[k, me, u] = jnp.dot(hid[u], w2[slot, u], preferred_element_type=F32).astype(BF16)

    w1_copy(0, 0).wait()
    up(0, 0)
    w1_copy(W_SLOTS, 0).start(priority=1)

    def step(k, carry):
        @pl.when(k >= 1)
        def _():
            send_own(Slots, k - 1)

        @pl.when(k >= LAG)
        def _():
            relay_near(Slots, k - LAG)

        slot, after = lax.rem(k, W_SLOTS), lax.rem(k + 1, W_SLOTS)
        w2_copy(k, slot).wait()
        w1_copy(k + 1, after).wait()
        down(k, slot)
        up(k + 1, after)

        @pl.when(k + W_SLOTS < n_chunk)
        def _():
            w2_copy(k + W_SLOTS, slot).start(priority=1)

        @pl.when(k + 1 + W_SLOTS < n_chunk)
        def _():
            w1_copy(k + 1 + W_SLOTS, after).start(priority=1)
        return carry

    lax.fori_loop(0, n_chunk - 1, step, 0)
    last = n_chunk - 1
    send_own(Slots, last - 1)
    w2_copy(last, last % W_SLOTS).wait()
    down(last, last % W_SLOTS)

    acc = jnp.zeros((own_tok, d_model), F32)

    def combine(acc, k):
        Slots.arrived(PARTNER, k)
        Slots.arrived(PARTNER_FAR, k)
        y = yg[k].reshape(n_dev * CHUNK * rows, d_model)
        return acc + jnp.dot(cexp[k], y, preferred_element_type=F32)

    first = last - LAG
    send_own(Slots, last)
    relay_near(Slots, first)
    far_done = comb_done = 0
    for k in range(first + 1, n_chunk):
        relay_near(Slots, k)
        for _ in range(2):
            if far_done < first - 1:
                relay_far(Slots, far_done)
                far_done += 1
                if far_done >= 3:
                    acc = combine(acc, comb_done)
                    comb_done += 1
    while far_done < n_chunk:
        relay_far(Slots, far_done)
        far_done += 1
        if far_done >= comb_done + 3:
            acc = combine(acc, comb_done)
            comb_done += 1
    while comb_done < n_chunk:
        acc = combine(acc, comb_done)
        comb_done += 1

    y = (acc * rowinv[...]).reshape(n_seq, n_tok, d_model)
    tpos = lax.broadcasted_iota(jnp.int32, (n_tok, d_model), 0) + me * n_tok
    for b in range(n_seq):
        out[b] = jnp.where(tpos < lens[b], y[b], 0.0).astype(BF16)

    Tokens.all_sent()
    Slots.all_sent()


def solution(mesh):
    n_dev = mesh.shape["seq"]

    def local_layer(tok_blk, len_blk, slot_param, logit_scale, w_in, w_out):
        n_seq, n_tok, d_model = tok_blk.shape
        n_exp, _, d_ff = w_in.shape
        n_slot = slot_param.shape[1]
        per_exp = n_slot // n_dev // n_exp
        rows = n_seq * per_exp
        n_chunk = n_exp // CHUNK
        vmem = pl.BlockSpec(memory_space=pltpu.VMEM)
        smem = pl.BlockSpec(memory_space=pltpu.SMEM)
        hbm = pl.BlockSpec(memory_space=pl.ANY)
        return pl.pallas_call(
            functools.partial(kernel, n_dev),
            out_shape=jax.ShapeDtypeStruct(tok_blk.shape, BF16),
            in_specs=[hbm, hbm, hbm, smem, hbm, hbm],
            out_specs=vmem,
            scratch_shapes=[
                pltpu.VMEM(tok_blk.shape, BF16),
                pltpu.VMEM(slot_param.shape, BF16),
                pltpu.SMEM(len_blk.shape, jnp.int32),
                pltpu.VMEM((n_seq, n_dev, n_tok, d_model), BF16),
                pltpu.VMEM((n_chunk, n_dev, CHUNK, rows, d_model), BF16),
                pltpu.VMEM((W_SLOTS, CHUNK, d_model, d_ff), BF16),
                pltpu.VMEM((W_SLOTS, CHUNK, d_ff, d_model), BF16),
                pltpu.VMEM((d_model // LANES, n_slot, LANES), F32),
                pltpu.VMEM((d_model // LANES, n_slot, LANES), F32),
                pltpu.VMEM((n_seq, n_slot // n_dev, ACROSS * n_tok), F32),
                pltpu.VMEM((n_chunk, n_seq * n_tok, n_dev * CHUNK * rows), BF16),
                pltpu.VMEM((CHUNK, rows, d_ff), BF16),
                pltpu.VMEM((n_seq * n_tok, 1), F32),
                pltpu.SemaphoreType.DMA((3,)),
                pltpu.SemaphoreType.DMA((W_SLOTS,)),
                pltpu.SemaphoreType.DMA((W_SLOTS,)),
                pltpu.SemaphoreType.DMA,
                pltpu.SemaphoreType.DMA((5, n_seq // SEQ_CHUNK)),
                pltpu.SemaphoreType.DMA,
                pltpu.SemaphoreType.DMA((5, n_chunk)),
            ],
            compiler_params=pltpu.CompilerParams(collective_id=0, has_side_effects=True, vmem_limit_bytes=67000000),
            name="soft_moe",
        )(tok_blk, len_blk, slot_param, logit_scale.reshape(1), w_in, w_out)

    return jax.shard_map(local_layer, mesh=mesh, in_specs=(P("data", "seq", None), P("data"), P(None, None), P(), P("seq", None, None), P("seq", None, None)), out_specs=P("data", "seq", None), check_vma=False)
```

```python
import functools

import jax
import jax.numpy as jnp
from jax import lax
from jax.experimental import pallas as pl
from jax.experimental.pallas import tpu as pltpu
from jax.sharding import PartitionSpec as P

EPSILON = 1e-6
NEG_FILL = -1e30
F32 = jnp.float32
BF16 = jnp.bfloat16
LANES = 128
MESH = pl.DeviceIdType.MESH

OWN_R, OWN_L, OWN_P, FWD_R, FWD_L, FWD_R2, FWD_L2, L_TO_P, R_TO_P, FAR_TO_P = range(10)
UNITS_SENT = 7
FROM_LEFT, FROM_RIGHT, FAR, PARTNER, PARTNER_FAR = range(5)
RECV = {OWN_R: FROM_LEFT, OWN_L: FROM_RIGHT, FWD_R: FAR, FWD_L: FAR, FWD_R2: PARTNER_FAR, FWD_L2: PARTNER_FAR, FAR_TO_P: PARTNER_FAR}
UNITS = {PARTNER: 3}
OWN, LEFT, RIGHT, ACROSS = 0, 2, 4, 6
SRC_PLACE = {FWD_R: LEFT, FWD_L: RIGHT, FWD_R2: LEFT, FWD_L2: RIGHT, L_TO_P: LEFT, R_TO_P: RIGHT, FAR_TO_P: ACROSS}
DST_PLACE = {OWN_R: LEFT, OWN_L: RIGHT, OWN_P: OWN + 1, FWD_R: ACROSS, FWD_L: ACROSS, FWD_R2: ACROSS + 1, FWD_L2: ACROSS + 1, L_TO_P: LEFT + 1, R_TO_P: RIGHT + 1, FAR_TO_P: ACROSS + 1}

CHUNK = 4
W_SLOTS = 5
SEQ_CHUNK = 2
TOK_BOTH = 2
SLOT_BOTH = 6
LAG = 4


def unit(values, axis):
    v = values.astype(F32)
    return v * lax.rsqrt(jnp.sum(v * v, axis=axis, keepdims=True) + EPSILON)


def kernel(n_dev, tok_hbm, lens_hbm, phi_hbm, gain, w_in, w_out, out,
           tok, phi, lens, xg, yg, w1, w2, xs, pnt, nlt, cexp, hid, rowinv,
           insem, sem1, sem2, tsend, trecv, ysend, yrecv):
    n_seq, n_tok, d_model = tok.shape
    n_exp = w_in.shape[0]
    n_slot = phi.shape[1]
    per_dev = n_slot // n_dev
    per_exp = per_dev // n_exp
    rows = n_seq * per_exp
    n_chunk = n_exp // CHUNK
    n_tchunk = n_seq // SEQ_CHUNK
    n_chip = n_dev // 2
    own_tok = n_seq * n_tok
    slabs = d_model // LANES

    me = lax.axis_index("seq")
    chip, core = me // 2, lax.rem(me, 2)
    right = lax.rem(chip + 1, n_chip) * 2 + core
    left = lax.rem(chip + n_chip - 1, n_chip) * 2 + core
    far = lax.rem(chip + 2, n_chip) * 2 + core
    partner = chip * 2 + 1 - core

    barrier = pltpu.get_barrier_semaphore()
    other = 1 - 2 * core
    for peer in (right, left, right + other, left + other, partner):
        pl.semaphore_signal(barrier, inc=1, device_id={"seq": peer}, device_id_type=MESH)

    tok_in = pltpu.make_async_copy(tok_hbm, tok, insem.at[0])
    phi_in = pltpu.make_async_copy(phi_hbm, phi, insem.at[1])
    lens_in = pltpu.make_async_copy(lens_hbm, lens, insem.at[2])
    tok_in.start()
    phi_in.start()
    lens_in.start()

    def w1_copy(k, slot):
        return pltpu.make_async_copy(w_in.at[pl.ds(k * CHUNK, CHUNK)], w1.at[slot], sem1.at[slot])

    def w2_copy(k, slot):
        return pltpu.make_async_copy(w_out.at[pl.ds(k * CHUNK, CHUNK)], w2.at[slot], sem2.at[slot])

    for k in range(W_SLOTS):
        w1_copy(k, k).start(priority=1)
        w2_copy(k, k).start(priority=1)

    dest = {OWN_R: right, OWN_L: left, FWD_R: right, FWD_L: left, FWD_R2: right + other, FWD_L2: left + other}
    origins = {FWD_R: left, FWD_L: right, FWD_R2: left, FWD_L2: right, L_TO_P: left, R_TO_P: right, FAR_TO_P: far}

    def part(kind, size):
        if kind in (FWD_R, FWD_R2):
            return 0, size // 2
        if kind in (FWD_L, FWD_L2):
            return size // 2, size // 2
        return 0, size

    def remote(src, dst, send_sem, recv_sem, device):
        return pltpu.make_async_remote_copy(src_ref=src, dst_ref=dst, send_sem=send_sem, recv_sem=recv_sem,
                                            device_id={"seq": device}, device_id_type=MESH)

    class Tokens:
        both = TOK_BOTH

        def send(kind, k):
            lo, num = part(kind, SEQ_CHUNK)
            lo = lo + k * SEQ_CHUNK
            dst = xg.at[pl.ds(lo, num), DST_PLACE[kind]]
            src = xg.at[pl.ds(lo, num), SRC_PLACE[kind]] if kind in SRC_PLACE else tok.at[pl.ds(lo, num)]
            remote(src, dst, tsend, trecv.at[RECV.get(kind, PARTNER), k], dest.get(kind, partner)).start()

        def arrived(what, k):
            ref = xg.at[pl.ds(k * SEQ_CHUNK, SEQ_CHUNK), pl.ds(0, UNITS.get(what, 1))]
            remote(ref, ref, tsend, trecv.at[what, k], partner).wait_recv()

        def all_sent():
            ref = xg.at[:, pl.ds(0, UNITS_SENT)]
            remote(ref, ref, tsend, trecv.at[0, 0], partner).wait_send()

    class Slots:
        both = SLOT_BOTH

        def send(kind, k):
            lo, num = part(kind, CHUNK)
            ref = yg.at[k, origins.get(kind, me), pl.ds(lo, num)]
            remote(ref, ref, ysend, yrecv.at[RECV.get(kind, PARTNER), k], dest.get(kind, partner)).start()

        def arrived(what, k):
            ref = yg.at[k, pl.ds(0, UNITS.get(what, 1))]
            remote(ref, ref, ysend, yrecv.at[what, k], partner).wait_recv()

        def all_sent():
            ref = yg.at[:, pl.ds(0, UNITS_SENT)]
            remote(ref, ref, ysend, yrecv.at[0, 0], partner).wait_send()

    def send_own(gather, k):
        for kind in (OWN_R, OWN_L, OWN_P):
            gather.send(kind, k)

    def relay_near(gather, k):
        both = isinstance(k, int) and k >= gather.both
        gather.arrived(FROM_LEFT, k)
        gather.send(FWD_R, k)
        if both:
            gather.send(FWD_R2, k)
        gather.send(L_TO_P, k)
        gather.arrived(FROM_RIGHT, k)
        gather.send(FWD_L, k)
        if both:
            gather.send(FWD_L2, k)
        gather.send(R_TO_P, k)

    def relay_far(gather, k):
        gather.arrived(FAR, k)
        if k < gather.both:
            gather.send(FAR_TO_P, k)

    tok_in.wait()
    pl.semaphore_wait(barrier, 5)
    for k in range(n_tchunk):
        send_own(Tokens, k)

    for b in range(n_seq):
        xg[b, OWN] = tok[b]

    phi_in.wait()
    lens_in.wait()
    g = gain[0]
    pn = unit(phi[...], 0).astype(BF16)
    pnt32 = pn.astype(F32).T
    for j in range(slabs):
        pnt[j] = pnt32[:, j * LANES:(j + 1) * LANES]

    def strided_rows(ref, start, size, stride):
        return jnp.concatenate([ref[j, pl.ds(start, size, stride=stride), :] for j in range(slabs)], axis=1)

    own_rows = jnp.concatenate([strided_rows(pnt, me * per_dev + s, n_exp, per_exp) for s in range(per_exp)], axis=0).astype(BF16)

    own = tok[...].reshape(own_tok, d_model)
    own_unit = unit(own, 1).astype(BF16)
    logits = g * jnp.dot(own_unit, pn, preferred_element_type=F32)
    comb = jnp.exp(logits - jnp.max(logits, axis=1, keepdims=True))
    rowinv[...] = 1.0 / jnp.sum(comb, axis=1, keepdims=True)
    comb = comb.astype(BF16)

    relay_near(Tokens, 0)

    width = 256
    devs = width // (CHUNK * rows)
    src = lax.broadcasted_iota(jnp.int32, (devs * per_dev, width), 0)
    col = lax.broadcasted_iota(jnp.int32, (devs * per_dev, width), 1)
    base = col // (CHUNK * rows) * per_dev + lax.rem(col, CHUNK * rows) // rows * per_exp + lax.rem(col, per_exp)
    row_seq = lax.broadcasted_iota(jnp.int32, (own_tok, width), 0) // n_tok
    col_seq = lax.rem(lax.broadcasted_iota(jnp.int32, (own_tok, width), 1), rows) // per_exp
    same = row_seq == col_seq

    def spread(k):
        pick = (src == base + k * (CHUNK * per_exp)).astype(F32).astype(BF16)
        for d in range(n_dev // devs):
            piece = jnp.dot(comb[:, d * devs * per_dev:(d + 1) * devs * per_dev], pick, preferred_element_type=F32)
            cexp[k, :, d * width:(d + 1) * width] = jnp.where(same, piece, 0.0).astype(BF16)

    share = n_chunk // (n_tchunk - 1)
    for t in range(1, n_tchunk):
        for k in range((t - 1) * share, n_chunk if t == n_tchunk - 1 else t * share):
            spread(k)
        relay_near(Tokens, t)

    near = ACROSS
    places = (me, partner, left, left + other, right, right + other, far, far + other)

    def positions(first, last):
        lane = lax.broadcasted_iota(jnp.int32, (per_dev, (last - first) * n_tok), 1)
        device = jnp.full(lane.shape, places[first], jnp.int32)
        for r in range(first + 1, last):
            device = jnp.where(lane // n_tok == r - first, places[r], device)
        return device * n_tok + lax.rem(lane, n_tok)

    def part_logits(x, pos, b):
        xn = unit(x, 1).astype(BF16)
        lt = g * lax.dot_general(own_rows, xn, (((1,), (1,)), ((), ())), preferred_element_type=F32)
        return jnp.where(pos < lens[b], lt, NEG_FILL)

    near_pos, far_pos = positions(0, near), positions(near, n_dev)

    def tokens_of(b, first, last):
        return xg[b, first:last].reshape((last - first) * n_tok, d_model)

    def near_logits(k):
        Tokens.arrived(PARTNER, k)
        for b in range(k * SEQ_CHUNK, (k + 1) * SEQ_CHUNK):
            nlt[b] = part_logits(tokens_of(b, 0, near), near_pos, b)

    def dispatch(b):
        lt_n, x_f = nlt[b], tokens_of(b, near, n_dev)
        lt_f = part_logits(x_f, far_pos, b)
        top = jnp.maximum(jnp.max(lt_n, axis=1, keepdims=True), jnp.max(lt_f, axis=1, keepdims=True))
        e_n, e_f = jnp.exp(lt_n - top), jnp.exp(lt_f - top)
        z = jnp.sum(e_n, axis=1, keepdims=True) + jnp.sum(e_f, axis=1, keepdims=True)
        s = jnp.dot(e_n.astype(BF16), tokens_of(b, 0, near), preferred_element_type=F32)
        s = (s + jnp.dot(e_f.astype(BF16), x_f, preferred_element_type=F32)) / z
        s = s.astype(BF16).astype(F32)
        for j in range(slabs):
            xs[j, b * per_dev:(b + 1) * per_dev, :] = s[:, j * LANES:(j + 1) * LANES]

    def dispatch_chunks(first, last):
        for k in range(first, last):
            if k >= Tokens.both:
                relay_far(Tokens, k)
            Tokens.arrived(PARTNER_FAR, k)
        for b in range(first * SEQ_CHUNK, last * SEQ_CHUNK):
            dispatch(b)

    for k in range(n_tchunk):
        near_logits(k)
        if 1 <= k <= Tokens.both:
            relay_far(Tokens, k - 1)
    dispatch_chunks(0, 2)
    dispatch_chunks(2, n_tchunk)

    def up(k, slot):
        for u in range(CHUNK):
            x = strided_rows(xs, k * CHUNK + u, rows, n_exp).astype(BF16)
            hid[u] = jax.nn.gelu(jnp.dot(x, w1[slot, u], preferred_element_type=F32)).astype(BF16)

    def down(k, slot):
        for u in range(CHUNK):
            yg[k, me, u] = jnp.dot(hid[u], w2[slot, u], preferred_element_type=F32).astype(BF16)

    w1_copy(0, 0).wait()
    up(0, 0)
    w1_copy(W_SLOTS, 0).start(priority=1)

    def step(k, carry):
        @pl.when(k >= 1)
        def _():
            send_own(Slots, k - 1)

        @pl.when(k >= LAG)
        def _():
            relay_near(Slots, k - LAG)

        slot, after = lax.rem(k, W_SLOTS), lax.rem(k + 1, W_SLOTS)
        w2_copy(k, slot).wait()
        w1_copy(k + 1, after).wait()
        down(k, slot)
        up(k + 1, after)

        @pl.when(k + W_SLOTS < n_chunk)
        def _():
            w2_copy(k + W_SLOTS, slot).start(priority=1)

        @pl.when(k + 1 + W_SLOTS < n_chunk)
        def _():
            w1_copy(k + 1 + W_SLOTS, after).start(priority=1)
        return carry

    lax.fori_loop(0, n_chunk - 1, step, 0)
    last = n_chunk - 1
    send_own(Slots, last - 1)
    w2_copy(last, last % W_SLOTS).wait()
    down(last, last % W_SLOTS)

    acc = jnp.zeros((own_tok, d_model), F32)

    def combine(acc, k):
        Slots.arrived(PARTNER, k)
        Slots.arrived(PARTNER_FAR, k)
        y = yg[k].reshape(n_dev * CHUNK * rows, d_model)
        return acc + jnp.dot(cexp[k], y, preferred_element_type=F32)

    first = last - LAG
    send_own(Slots, last)
    relay_near(Slots, first)
    far_done = comb_done = 0
    for k in range(first + 1, n_chunk):
        relay_near(Slots, k)
        for _ in range(2):
            if far_done < first - 1:
                relay_far(Slots, far_done)
                far_done += 1
                if far_done >= 3:
                    acc = combine(acc, comb_done)
                    comb_done += 1
    while far_done < n_chunk:
        relay_far(Slots, far_done)
        far_done += 1
        if far_done >= comb_done + 3:
            acc = combine(acc, comb_done)
            comb_done += 1
    while comb_done < n_chunk:
        acc = combine(acc, comb_done)
        comb_done += 1

    y = (acc * rowinv[...]).reshape(n_seq, n_tok, d_model)
    tpos = lax.broadcasted_iota(jnp.int32, (n_tok, d_model), 0) + me * n_tok
    for b in range(n_seq):
        out[b] = jnp.where(tpos < lens[b], y[b], 0.0).astype(BF16)

    Tokens.all_sent()
    Slots.all_sent()


def solution(mesh):
    n_dev = mesh.shape["seq"]

    def local_layer(tok_blk, len_blk, slot_param, logit_scale, w_in, w_out):
        n_seq, n_tok, d_model = tok_blk.shape
        n_exp, _, d_ff = w_in.shape
        n_slot = slot_param.shape[1]
        per_exp = n_slot // n_dev // n_exp
        rows = n_seq * per_exp
        n_chunk = n_exp // CHUNK
        vmem = pl.BlockSpec(memory_space=pltpu.VMEM)
        smem = pl.BlockSpec(memory_space=pltpu.SMEM)
        hbm = pl.BlockSpec(memory_space=pl.ANY)
        return pl.pallas_call(
            functools.partial(kernel, n_dev),
            out_shape=jax.ShapeDtypeStruct(tok_blk.shape, BF16),
            in_specs=[hbm, hbm, hbm, smem, hbm, hbm],
            out_specs=vmem,
            scratch_shapes=[
                pltpu.VMEM(tok_blk.shape, BF16),
                pltpu.VMEM(slot_param.shape, BF16),
                pltpu.SMEM(len_blk.shape, jnp.int32),
                pltpu.VMEM((n_seq, n_dev, n_tok, d_model), BF16),
                pltpu.VMEM((n_chunk, n_dev, CHUNK, rows, d_model), BF16),
                pltpu.VMEM((W_SLOTS, CHUNK, d_model, d_ff), BF16),
                pltpu.VMEM((W_SLOTS, CHUNK, d_ff, d_model), BF16),
                pltpu.VMEM((d_model // LANES, n_slot, LANES), F32),
                pltpu.VMEM((d_model // LANES, n_slot, LANES), F32),
                pltpu.VMEM((n_seq, n_slot // n_dev, ACROSS * n_tok), F32),
                pltpu.VMEM((n_chunk, n_seq * n_tok, n_dev * CHUNK * rows), BF16),
                pltpu.VMEM((CHUNK, rows, d_ff), BF16),
                pltpu.VMEM((n_seq * n_tok, 1), F32),
                pltpu.SemaphoreType.DMA((3,)),
                pltpu.SemaphoreType.DMA((W_SLOTS,)),
                pltpu.SemaphoreType.DMA((W_SLOTS,)),
                pltpu.SemaphoreType.DMA,
                pltpu.SemaphoreType.DMA((5, n_seq // SEQ_CHUNK)),
                pltpu.SemaphoreType.DMA,
                pltpu.SemaphoreType.DMA((5, n_chunk)),
            ],
            compiler_params=pltpu.CompilerParams(collective_id=0, has_side_effects=True, vmem_limit_bytes=67000000),
            name="soft_moe",
        )(tok_blk, len_blk, slot_param, logit_scale.reshape(1), w_in, w_out)

    return jax.shard_map(local_layer, mesh=mesh, in_specs=(P("data", "seq", None), P("data"), P(None, None), P(), P("seq", None, None), P("seq", None, None)), out_specs=P("data", "seq", None), check_vma=False)
```

```python
import functools

import jax
import jax.numpy as jnp
from jax import lax
from jax.experimental import pallas as pl
from jax.experimental.pallas import tpu as pltpu
from jax.sharding import PartitionSpec as P

EPSILON = 1e-6
NEG_FILL = -1e30
F32 = jnp.float32
BF16 = jnp.bfloat16
LANES = 128
MESH = pl.DeviceIdType.MESH

OWN_R, OWN_L, OWN_P, FWD_R, FWD_L, FWD_R2, FWD_L2, L_TO_P, R_TO_P, FAR_TO_P = range(10)
UNITS_SENT = 7
FROM_LEFT, FROM_RIGHT, FAR, PARTNER, PARTNER_FAR = range(5)
RECV = {OWN_R: FROM_LEFT, OWN_L: FROM_RIGHT, FWD_R: FAR, FWD_L: FAR, FWD_R2: PARTNER_FAR, FWD_L2: PARTNER_FAR, FAR_TO_P: PARTNER_FAR}
UNITS = {PARTNER: 3}
OWN, LEFT, RIGHT, ACROSS = 0, 2, 4, 6
SRC_PLACE = {FWD_R: LEFT, FWD_L: RIGHT, FWD_R2: LEFT, FWD_L2: RIGHT, L_TO_P: LEFT, R_TO_P: RIGHT, FAR_TO_P: ACROSS}
DST_PLACE = {OWN_R: LEFT, OWN_L: RIGHT, OWN_P: OWN + 1, FWD_R: ACROSS, FWD_L: ACROSS, FWD_R2: ACROSS + 1, FWD_L2: ACROSS + 1, L_TO_P: LEFT + 1, R_TO_P: RIGHT + 1, FAR_TO_P: ACROSS + 1}

CHUNK = 4
W_SLOTS = 5
SEQ_CHUNK = 2
TOK_BOTH = 2
SLOT_BOTH = 6
LAG = 4


def unit(values, axis):
    v = values.astype(F32)
    return v * lax.rsqrt(jnp.sum(v * v, axis=axis, keepdims=True) + EPSILON)


def kernel(n_dev, tok_hbm, lens_hbm, phi_hbm, gain, w_in, w_out, out,
           tok, phi, lens, xg, yg, w1, w2, xs, pnt, nlt, cexp, hid, rowinv,
           insem, sem1, sem2, tsend, trecv, ysend, yrecv):
    n_seq, n_tok, d_model = tok.shape
    n_exp = w_in.shape[0]
    n_slot = phi.shape[1]
    per_dev = n_slot // n_dev
    per_exp = per_dev // n_exp
    rows = n_seq * per_exp
    n_chunk = n_exp // CHUNK
    n_tchunk = n_seq // SEQ_CHUNK
    n_chip = n_dev // 2
    own_tok = n_seq * n_tok
    slabs = d_model // LANES

    me = lax.axis_index("seq")
    chip, core = me // 2, lax.rem(me, 2)
    right = lax.rem(chip + 1, n_chip) * 2 + core
    left = lax.rem(chip + n_chip - 1, n_chip) * 2 + core
    far = lax.rem(chip + 2, n_chip) * 2 + core
    partner = chip * 2 + 1 - core

    barrier = pltpu.get_barrier_semaphore()
    other = 1 - 2 * core
    for peer in (right, left, right + other, left + other, partner):
        pl.semaphore_signal(barrier, inc=1, device_id={"seq": peer}, device_id_type=MESH)

    tok_in = pltpu.make_async_copy(tok_hbm, tok, insem.at[0])
    phi_in = pltpu.make_async_copy(phi_hbm, phi, insem.at[1])
    lens_in = pltpu.make_async_copy(lens_hbm, lens, insem.at[2])
    tok_in.start()
    phi_in.start()
    lens_in.start()

    def w1_copy(k, slot):
        return pltpu.make_async_copy(w_in.at[pl.ds(k * CHUNK, CHUNK)], w1.at[slot], sem1.at[slot])

    def w2_copy(k, slot):
        return pltpu.make_async_copy(w_out.at[pl.ds(k * CHUNK, CHUNK)], w2.at[slot], sem2.at[slot])

    for k in range(W_SLOTS):
        w1_copy(k, k).start(priority=1)
        w2_copy(k, k).start(priority=1)

    dest = {OWN_R: right, OWN_L: left, FWD_R: right, FWD_L: left, FWD_R2: right + other, FWD_L2: left + other}
    origins = {FWD_R: left, FWD_L: right, FWD_R2: left, FWD_L2: right, L_TO_P: left, R_TO_P: right, FAR_TO_P: far}

    def part(kind, size):
        if kind in (FWD_R, FWD_R2):
            return 0, size // 2
        if kind in (FWD_L, FWD_L2):
            return size // 2, size // 2
        return 0, size

    def remote(src, dst, send_sem, recv_sem, device):
        return pltpu.make_async_remote_copy(src_ref=src, dst_ref=dst, send_sem=send_sem, recv_sem=recv_sem,
                                            device_id={"seq": device}, device_id_type=MESH)

    class Tokens:
        both = TOK_BOTH

        def send(kind, k):
            lo, num = part(kind, SEQ_CHUNK)
            lo = lo + k * SEQ_CHUNK
            dst = xg.at[pl.ds(lo, num), DST_PLACE[kind]]
            src = xg.at[pl.ds(lo, num), SRC_PLACE[kind]] if kind in SRC_PLACE else tok.at[pl.ds(lo, num)]
            remote(src, dst, tsend, trecv.at[RECV.get(kind, PARTNER), k], dest.get(kind, partner)).start()

        def arrived(what, k):
            ref = xg.at[pl.ds(k * SEQ_CHUNK, SEQ_CHUNK), pl.ds(0, UNITS.get(what, 1))]
            remote(ref, ref, tsend, trecv.at[what, k], partner).wait_recv()

        def all_sent():
            ref = xg.at[:, pl.ds(0, UNITS_SENT)]
            remote(ref, ref, tsend, trecv.at[0, 0], partner).wait_send()

    class Slots:
        both = SLOT_BOTH

        def send(kind, k):
            lo, num = part(kind, CHUNK)
            ref = yg.at[k, origins.get(kind, me), pl.ds(lo, num)]
            remote(ref, ref, ysend, yrecv.at[RECV.get(kind, PARTNER), k], dest.get(kind, partner)).start()

        def arrived(what, k):
            ref = yg.at[k, pl.ds(0, UNITS.get(what, 1))]
            remote(ref, ref, ysend, yrecv.at[what, k], partner).wait_recv()

        def all_sent():
            ref = yg.at[:, pl.ds(0, UNITS_SENT)]
            remote(ref, ref, ysend, yrecv.at[0, 0], partner).wait_send()

    def send_own(gather, k):
        for kind in (OWN_R, OWN_L, OWN_P):
            gather.send(kind, k)

    def relay_near(gather, k):
        both = isinstance(k, int) and k >= gather.both
        gather.arrived(FROM_LEFT, k)
        gather.send(FWD_R, k)
        if both:
            gather.send(FWD_R2, k)
        gather.send(L_TO_P, k)
        gather.arrived(FROM_RIGHT, k)
        gather.send(FWD_L, k)
        if both:
            gather.send(FWD_L2, k)
        gather.send(R_TO_P, k)

    def relay_far(gather, k):
        gather.arrived(FAR, k)
        if k < gather.both:
            gather.send(FAR_TO_P, k)

    tok_in.wait()
    pl.semaphore_wait(barrier, 5)
    for k in range(n_tchunk):
        send_own(Tokens, k)

    for b in range(n_seq):
        xg[b, OWN] = tok[b]

    phi_in.wait()
    lens_in.wait()
    g = gain[0]
    pn = unit(phi[...], 0).astype(BF16)
    pnt32 = pn.astype(F32).T
    for j in range(slabs):
        pnt[j] = pnt32[:, j * LANES:(j + 1) * LANES]

    def strided_rows(ref, start, size, stride):
        return jnp.concatenate([ref[j, pl.ds(start, size, stride=stride), :] for j in range(slabs)], axis=1)

    own_rows = jnp.concatenate([strided_rows(pnt, me * per_dev + s, n_exp, per_exp) for s in range(per_exp)], axis=0).astype(BF16)

    own = tok[...].reshape(own_tok, d_model)
    own_unit = unit(own, 1).astype(BF16)
    logits = g * jnp.dot(own_unit, pn, preferred_element_type=F32)
    comb = jnp.exp(logits - jnp.max(logits, axis=1, keepdims=True))
    rowinv[...] = 1.0 / jnp.sum(comb, axis=1, keepdims=True)
    comb = comb.astype(BF16)

    relay_near(Tokens, 0)

    width = 256
    devs = width // (CHUNK * rows)
    src = lax.broadcasted_iota(jnp.int32, (devs * per_dev, width), 0)
    col = lax.broadcasted_iota(jnp.int32, (devs * per_dev, width), 1)
    base = col // (CHUNK * rows) * per_dev + lax.rem(col, CHUNK * rows) // rows * per_exp + lax.rem(col, per_exp)
    row_seq = lax.broadcasted_iota(jnp.int32, (own_tok, width), 0) // n_tok
    col_seq = lax.rem(lax.broadcasted_iota(jnp.int32, (own_tok, width), 1), rows) // per_exp
    same = row_seq == col_seq

    def spread(k):
        pick = (src == base + k * (CHUNK * per_exp)).astype(F32).astype(BF16)
        for d in range(n_dev // devs):
            piece = jnp.dot(comb[:, d * devs * per_dev:(d + 1) * devs * per_dev], pick, preferred_element_type=F32)
            cexp[k, :, d * width:(d + 1) * width] = jnp.where(same, piece, 0.0).astype(BF16)

    share = n_chunk // (n_tchunk - 1)
    for t in range(1, n_tchunk):
        for k in range((t - 1) * share, n_chunk if t == n_tchunk - 1 else t * share):
            spread(k)
        relay_near(Tokens, t)

    near = ACROSS
    places = (me, partner, left, left + other, right, right + other, far, far + other)

    def positions(first, last):
        lane = lax.broadcasted_iota(jnp.int32, (per_dev, (last - first) * n_tok), 1)
        device = jnp.full(lane.shape, places[first], jnp.int32)
        for r in range(first + 1, last):
            device = jnp.where(lane // n_tok == r - first, places[r], device)
        return device * n_tok + lax.rem(lane, n_tok)

    def part_logits(x, pos, b):
        xn = unit(x, 1).astype(BF16)
        lt = g * lax.dot_general(own_rows, xn, (((1,), (1,)), ((), ())), preferred_element_type=F32)
        return jnp.where(pos < lens[b], lt, NEG_FILL)

    near_pos, far_pos = positions(0, near), positions(near, n_dev)

    def tokens_of(b, first, last):
        return xg[b, first:last].reshape((last - first) * n_tok, d_model)

    def near_logits(k):
        Tokens.arrived(PARTNER, k)
        for b in range(k * SEQ_CHUNK, (k + 1) * SEQ_CHUNK):
            nlt[b] = part_logits(tokens_of(b, 0, near), near_pos, b)

    def dispatch(b):
        lt_n, x_f = nlt[b], tokens_of(b, near, n_dev)
        lt_f = part_logits(x_f, far_pos, b)
        top = jnp.maximum(jnp.max(lt_n, axis=1, keepdims=True), jnp.max(lt_f, axis=1, keepdims=True))
        e_n, e_f = jnp.exp(lt_n - top), jnp.exp(lt_f - top)
        z = jnp.sum(e_n, axis=1, keepdims=True) + jnp.sum(e_f, axis=1, keepdims=True)
        s = jnp.dot(e_n.astype(BF16), tokens_of(b, 0, near), preferred_element_type=F32)
        s = (s + jnp.dot(e_f.astype(BF16), x_f, preferred_element_type=F32)) / z
        s = s.astype(BF16).astype(F32)
        for j in range(slabs):
            xs[j, b * per_dev:(b + 1) * per_dev, :] = s[:, j * LANES:(j + 1) * LANES]

    def dispatch_chunks(first, last):
        for k in range(first, last):
            if k >= Tokens.both:
                relay_far(Tokens, k)
            Tokens.arrived(PARTNER_FAR, k)
        for b in range(first * SEQ_CHUNK, last * SEQ_CHUNK):
            dispatch(b)

    for k in range(n_tchunk):
        near_logits(k)
        if 1 <= k <= Tokens.both:
            relay_far(Tokens, k - 1)
    dispatch_chunks(0, 2)
    dispatch_chunks(2, n_tchunk)

    def up(k, slot, experts=range(CHUNK)):
        for u in experts:
            x = strided_rows(xs, k * CHUNK + u, rows, n_exp).astype(BF16)
            hid[u] = jax.nn.gelu(jnp.dot(x, w1[slot, u], preferred_element_type=F32)).astype(BF16)

    def down(k, slot):
        for u in range(CHUNK):
            yg[k, me, u] = jnp.dot(hid[u], w2[slot, u], preferred_element_type=F32).astype(BF16)

    w1_copy(0, 0).wait()
    up(0, 0)
    w1_copy(W_SLOTS, 0).start(priority=1)
    w2_copy(0, 0).wait()
    w1_copy(1, 1).wait()
    down(0, 0)
    up(1, 1, range(1))
    send_own(Slots, 0)
    up(1, 1, range(1, CHUNK))
    w2_copy(W_SLOTS, 0).start(priority=1)
    w1_copy(W_SLOTS + 1, 1).start(priority=1)

    def step(k, carry):
        @pl.when(k >= 2)
        def _():
            send_own(Slots, k - 1)

        @pl.when(k >= LAG)
        def _():
            relay_near(Slots, k - LAG)

        slot, after = lax.rem(k, W_SLOTS), lax.rem(k + 1, W_SLOTS)
        w2_copy(k, slot).wait()
        w1_copy(k + 1, after).wait()
        down(k, slot)
        up(k + 1, after)

        @pl.when(k + W_SLOTS < n_chunk)
        def _():
            w2_copy(k + W_SLOTS, slot).start(priority=1)

        @pl.when(k + 1 + W_SLOTS < n_chunk)
        def _():
            w1_copy(k + 1 + W_SLOTS, after).start(priority=1)
        return carry

    lax.fori_loop(1, n_chunk - 1, step, 0)
    last = n_chunk - 1
    send_own(Slots, last - 1)
    w2_copy(last, last % W_SLOTS).wait()
    down(last, last % W_SLOTS)

    acc = jnp.zeros((own_tok, d_model), F32)

    def combine(acc, k):
        Slots.arrived(PARTNER, k)
        Slots.arrived(PARTNER_FAR, k)
        y = yg[k].reshape(n_dev * CHUNK * rows, d_model)
        return acc + jnp.dot(cexp[k], y, preferred_element_type=F32)

    first = last - LAG
    send_own(Slots, last)
    relay_near(Slots, first)
    far_done = comb_done = 0
    for k in range(first + 1, n_chunk):
        relay_near(Slots, k)
        for _ in range(2):
            if far_done < first - 1:
                relay_far(Slots, far_done)
                far_done += 1
                if far_done >= 3:
                    acc = combine(acc, comb_done)
                    comb_done += 1
    while far_done < n_chunk:
        relay_far(Slots, far_done)
        far_done += 1
        if far_done >= comb_done + 3:
            acc = combine(acc, comb_done)
            comb_done += 1
    while comb_done < n_chunk:
        acc = combine(acc, comb_done)
        comb_done += 1

    y = (acc * rowinv[...]).reshape(n_seq, n_tok, d_model)
    tpos = lax.broadcasted_iota(jnp.int32, (n_tok, d_model), 0) + me * n_tok
    for b in range(n_seq):
        out[b] = jnp.where(tpos < lens[b], y[b], 0.0).astype(BF16)

    Tokens.all_sent()
    Slots.all_sent()


def solution(mesh):
    n_dev = mesh.shape["seq"]

    def local_layer(tok_blk, len_blk, slot_param, logit_scale, w_in, w_out):
        n_seq, n_tok, d_model = tok_blk.shape
        n_exp, _, d_ff = w_in.shape
        n_slot = slot_param.shape[1]
        per_exp = n_slot // n_dev // n_exp
        rows = n_seq * per_exp
        n_chunk = n_exp // CHUNK
        vmem = pl.BlockSpec(memory_space=pltpu.VMEM)
        smem = pl.BlockSpec(memory_space=pltpu.SMEM)
        hbm = pl.BlockSpec(memory_space=pl.ANY)
        return pl.pallas_call(
            functools.partial(kernel, n_dev),
            out_shape=jax.ShapeDtypeStruct(tok_blk.shape, BF16),
            in_specs=[hbm, hbm, hbm, smem, hbm, hbm],
            out_specs=vmem,
            scratch_shapes=[
                pltpu.VMEM(tok_blk.shape, BF16),
                pltpu.VMEM(slot_param.shape, BF16),
                pltpu.SMEM(len_blk.shape, jnp.int32),
                pltpu.VMEM((n_seq, n_dev, n_tok, d_model), BF16),
                pltpu.VMEM((n_chunk, n_dev, CHUNK, rows, d_model), BF16),
                pltpu.VMEM((W_SLOTS, CHUNK, d_model, d_ff), BF16),
                pltpu.VMEM((W_SLOTS, CHUNK, d_ff, d_model), BF16),
                pltpu.VMEM((d_model // LANES, n_slot, LANES), F32),
                pltpu.VMEM((d_model // LANES, n_slot, LANES), F32),
                pltpu.VMEM((n_seq, n_slot // n_dev, ACROSS * n_tok), F32),
                pltpu.VMEM((n_chunk, n_seq * n_tok, n_dev * CHUNK * rows), BF16),
                pltpu.VMEM((CHUNK, rows, d_ff), BF16),
                pltpu.VMEM((n_seq * n_tok, 1), F32),
                pltpu.SemaphoreType.DMA((3,)),
                pltpu.SemaphoreType.DMA((W_SLOTS,)),
                pltpu.SemaphoreType.DMA((W_SLOTS,)),
                pltpu.SemaphoreType.DMA,
                pltpu.SemaphoreType.DMA((5, n_seq // SEQ_CHUNK)),
                pltpu.SemaphoreType.DMA,
                pltpu.SemaphoreType.DMA((5, n_chunk)),
            ],
            compiler_params=pltpu.CompilerParams(collective_id=0, has_side_effects=True, vmem_limit_bytes=67000000),
            name="soft_moe",
        )(tok_blk, len_blk, slot_param, logit_scale.reshape(1), w_in, w_out)

    return jax.shard_map(local_layer, mesh=mesh, in_specs=(P("data", "seq", None), P("data"), P(None, None), P(), P("seq", None, None), P("seq", None, None)), out_specs=P("data", "seq", None), check_vma=False)
```
